32 devices in a mesh: rows: 8 (over z, x), cols: 4 (over y, core).
Axes of the slice: x: 2, y: 2, z: 4, core: 2. Of those that a mesh axis runs over, the one named last changes fastest.
Arguments:
- basis: bfloat16 [65536, 512], P('rows', 'cols'), may hold values from -6 to 6
- lower: bfloat16 [256, 256, 256], P('rows'), may hold values from -0.375 to 0.375
- diag: bfloat16 [256, 256, 256], P('rows'), may hold values from -0.375 to 0.375
- upper: bfloat16 [256, 256, 256], P('rows'), may hold values from -0.375 to 0.375
- inverse: bfloat16 [256, 256, 256], P('rows'), may hold values from -0.375 to 0.375
Outputs:
- ortho: bfloat16 [65536, 512], P('rows', 'cols')
- projected: float32 [512, 512], P(None, 'cols')
The draws below stay inside these ranges and needn't reach their ends.
All inputs are finite; a program needn't handle non-finite values.
Results may differ from the reference program's by a relative error of at most 0.0085.
Values may be sent and summed in bfloat16 or wider, within the bound.
A program may use at most 128 MiB of HBM per device.

```python
import jax
import jax.numpy as jnp
from jax import lax

BS = 256
K = 512
NB = 256
ORDER = 65536


def block_scale(stream_key, shape, shards, low, largest):
    def one(dim, shards_of):
        heights = jax.random.uniform(jax.random.fold_in(jax.random.fold_in(stream_key, 6), dim), (shards_of,), jnp.float32, low / len(shards), largest / len(shards))
        return jnp.repeat(jnp.exp(heights), shape[dim] // shards_of).reshape((-1,) + (1,) * (len(shape) - dim - 1))

    gain = one(*shards[0])
    for cut in shards[1:]:
        gain = gain * one(*cut)
    return gain


def scatter_about(key, extent, scale, reach, pieces=(), kind=jnp.bfloat16):
    array = scale * jax.random.normal(key, extent, jnp.float32)
    if pieces:
        array = array * block_scale(key, extent, pieces, -0.22, 0.18)
    return jnp.clip(array, -reach, reach).astype(kind)


def setup_inputs(seed: int = 0) -> dict:
    streams_of = jax.random.split(jax.random.key(seed), 6)
    return {
        "basis": scatter_about(streams_of[0], (ORDER, K), 1.0, 6.0, ((0, 8), (1, 4))),
        "lower": scatter_about(streams_of[1], (NB, BS, BS), BS ** -0.5, 0.375, ((0, 8),)),
        "diag": scatter_about(streams_of[2], (NB, BS, BS), BS ** -0.5, 0.375, ((0, 8),)),
        "upper": scatter_about(streams_of[3], (NB, BS, BS), BS ** -0.5, 0.375, ((0, 8),)),
        "inverse": scatter_about(streams_of[4], (NB, BS, BS), BS ** -0.5, 0.375, ((0, 8),)),
    }


def operate(field, lower, diag, upper, inverse):
    blocks = field.reshape(NB, BS, K).astype(jnp.float32)
    zero = jnp.zeros((1, BS, K), jnp.float32)
    before = jnp.concatenate([zero, blocks[:-1]], axis=0)
    after = jnp.concatenate([blocks[1:], zero], axis=0)
    mixed = jnp.einsum('bij,bjc->bic', lower.astype(jnp.float32), before)
    mixed = mixed + jnp.einsum('bij,bjc->bic', diag.astype(jnp.float32), blocks)
    mixed = mixed + jnp.einsum('bij,bjc->bic', upper.astype(jnp.float32), after)
    mixed = mixed.astype(jnp.bfloat16).astype(jnp.float32)
    result = jnp.einsum('bij,bjc->bic', inverse.astype(jnp.float32), mixed)
    return result.astype(jnp.bfloat16).reshape(NB * BS, K)

def reference(basis, lower, diag, upper, inverse):
    work = operate(basis, lower, diag, upper, inverse)
    gram = jnp.dot(work.T.astype(jnp.float32), work.astype(jnp.float32), preferred_element_type=jnp.float32)
    factor = jnp.linalg.cholesky(gram)
    identity = jnp.eye(K, dtype=jnp.float32)
    linv = lax.linalg.triangular_solve(factor, identity, left_side=True, lower=True)
    rinv = linv.T.astype(jnp.bfloat16)
    ortho = jnp.dot(work.astype(jnp.float32), rinv.astype(jnp.float32), preferred_element_type=jnp.float32).astype(jnp.bfloat16)
    image = operate(ortho, lower, diag, upper, inverse)
    projected = jnp.dot(ortho.T.astype(jnp.float32), image.astype(jnp.float32), preferred_element_type=jnp.float32)
    return (ortho, projected)
```

```python
import functools

import jax
import jax.numpy as jnp
from jax import lax
from jax.experimental import pallas as pl
from jax.experimental.pallas import tpu as pltpu
from jax.sharding import PartitionSpec as P

LANES = 128
MESH = pl.DeviceIdType.MESH
VMEM = pl.BlockSpec(memory_space=pltpu.VMEM)
ANY = pl.BlockSpec(memory_space=pl.ANY)
SUB = 8
HI = lax.Precision.HIGHEST

def factor_tile(block):
    size = block.shape[0]
    wide = (SUB, size)
    tiles = size // SUB
    row_of = lax.broadcasted_iota(jnp.int32, wide, 0)
    lane_of = lax.broadcasted_iota(jnp.int32, wide, 1)
    a = [block[t * SUB:(t + 1) * SUB, :] for t in range(tiles)]
    m = [jnp.where(lane_of == row_of + t * SUB, 1.0, 0.0).astype(jnp.float32) for t in range(tiles)]
    out = []
    for t in range(tiles):
        at, mt = a[t], m[t]
        base = t * SUB
        pivot = {}
        for i in range(SUB):
            for j in range(i + 1):
                pivot[i, j] = jnp.broadcast_to(at[i:i + 1, base + j:base + j + 1], wide)
        ra = [jnp.broadcast_to(at[i:i + 1, :], wide) for i in range(SUB)]
        rm = [jnp.broadcast_to(mt[i:i + 1, :], wide) for i in range(SUB)]
        last = t == tiles - 1
        unit = {}
        sa, sm = [None] * SUB, [None] * SUB
        fin = jnp.zeros(wide, jnp.float32)
        for j in range(SUB):
            d = pivot[j, j]
            root = lax.rsqrt(d)
            inv = 1.0 / d
            fin = jnp.where(row_of == j, rm[j] * root, fin)
            for i in range(j + 1, SUB):
                unit[i, j] = pivot[i, j] * inv
            for i in range(j + 1, SUB):
                for q in range(j + 1, i + 1):
                    pivot[i, q] = pivot[i, q] - unit[i, j] * pivot[q, j]
            for i in range(j + 1, SUB):
                if not last:
                    ra[i] = ra[i] - unit[i, j] * ra[j]
                rm[i] = rm[i] - unit[i, j] * rm[j]
            if not last:
                sa[j] = ra[j] * inv
                sm[j] = rm[j] * inv
        out.append(fin)
        if last:
            break
        for j in range(SUB - 1, -1, -1):
            for i in range(j):
                sa[i] = sa[i] - unit[j, i] * sa[j]
                sm[i] = sm[i] - unit[j, i] * sm[j]
        for s in range(t + 1, tiles):
            na, nm = a[s], m[s]
            for j in range(SUB):
                c = jnp.broadcast_to(a[s][:, base + j:base + j + 1], wide)
                na = na - c * sa[j]
                nm = nm - c * sm[j]
            a[s], m[s] = na, nm
    return jnp.concatenate(out, axis=0)

def inverse_upper_steps(work_ref, out_ref, panel_ref):
    n, size, _ = work_ref.shape
    order = n * size
    def step(b, carry):
        at = [work_ref[b, :, i * size:(i + 1) * size] for i in range(n)]
        block = at[0]
        for i in range(1, n):
            block = jnp.where(b == i, at[i], block)
        linv = factor_tile(block)
        y = lax.dot_general(linv, work_ref[b], (((1,), (0,)), ((), ())), precision=HI, preferred_element_type=jnp.float32)
        work_ref[b] = y
        for i in range(n):
            panel_ref[i] = y[:, i * size:(i + 1) * size]
        def below(i, c):
            work_ref[i] = work_ref[i] - lax.dot_general(panel_ref[i], y_ref[...], (((0,), (0,)), ((), ())), precision=HI, preferred_element_type=jnp.float32)
            return c
        y_ref = work_ref.at[b]
        lax.fori_loop(b + 1, n, below, 0)
        return carry
    lax.fori_loop(0, n, step, 0)
    for b in range(n):
        out_ref[:, b * size:(b + 1) * size] = work_ref[b, :, order:].T.astype(out_ref.dtype)

def unpack_kernel(packed_ref, out_ref, work_ref, panel_ref):
    n, size, _ = work_ref.shape
    order = n * size
    row = lax.broadcasted_iota(jnp.int32, (size, order), 0)
    lane = lax.broadcasted_iota(jnp.int32, (size, order), 1)
    place = 0
    for i in range(n):
        work_ref[i, :, :order] = jnp.zeros((size, order), jnp.float32)
        work_ref[i, :, order:] = jnp.where(lane == row + i * size, 1.0, 0.0).astype(jnp.float32)
        for j in range(i, n):
            work_ref[i, :, j * size:(j + 1) * size] = packed_ref[place * size:(place + 1) * size, :]
            place += 1
    inverse_upper_steps(work_ref, out_ref, panel_ref)


def inverse_upper(packed, order):
    n = order // LANES
    return pl.pallas_call(
        unpack_kernel,
        out_shape=jax.ShapeDtypeStruct((order, order), jnp.bfloat16),
        in_specs=[VMEM],
        out_specs=VMEM,
        scratch_shapes=[
            pltpu.VMEM((n, LANES, 2 * order), jnp.float32),
            pltpu.VMEM((n, LANES, LANES), jnp.float32),
        ],
        cost_estimate=pl.CostEstimate(
            flops=8 * order**3, bytes_accessed=8 * order * order, transcendentals=0
        ),
        name="inverse_upper",
    )(packed)


def dot(left, right):
    return jnp.dot(left, right, preferred_element_type=jnp.float32)


def inner(left, right):
    return lax.dot_general(
        left, right, (((0,), (0,)), ((), ())), preferred_element_type=jnp.float32
    )


def remote(src, dst, send, recv, **where):
    return pltpu.make_async_remote_copy(
        src_ref=src, dst_ref=dst, send_sem=send, recv_sem=recv, device_id=where, device_id_type=MESH
    )


def exchange(axis, count, me, source, target, arrived, send, recv):
    for step in range(1, count):
        peer = lax.rem(me + step, count)
        remote(source(peer), target(me), send.at[step], recv.at[me], **{axis: peer}).start()

    def finish():
        for step in range(1, count):
            peer = lax.rem(me + step, count)
            remote(
                source(peer), arrived(peer), send.at[step], recv.at[peer], **{axis: peer}
            ).wait()

    return finish


def apply_block(i, size, field, wl, wd, wu, wi):
    def at(k):
        return field[pl.ds(pl.multiple_of(k * size, size), size), :]

    mixed = dot(wl[i], at(i)) + dot(wd[i], at(i + 1)) + dot(wu[i], at(i + 2))
    return dot(wi[i], mixed.astype(jnp.bfloat16)).astype(jnp.bfloat16)


def fetch_blocks(parts, held, sem, first):
    count = held[0].shape[0]
    copies = [
        pltpu.make_async_copy(part.at[pl.ds(first * count, count)], ref, sem.at[k])
        for k, (part, ref) in enumerate(zip(parts, held))
    ]
    for copy in copies:
        copy.start()
    return copies


def front_kernel(
    nr, nc, basis, lower, diag, upper, inverse, wext, gram,
    field, wl, wd, wu, wi, total, packed, got1, part, got2,
    wsem, lsem, fsend, frecv, hsend, hrecv, s1, r1, s2, r2, s3, r3, s4, r4,
):
    r, c = lax.axis_index("rows"), lax.axis_index("cols")
    count, size, _ = wl.shape
    width = basis.shape[1]
    body = count * size
    top = (count + 1) * size
    share = got1.shape[1]
    piece = got2.shape[1]

    weights = fetch_blocks((lower, diag, upper, inverse), (wl, wd, wu, wi), wsem, c)

    def columns(k):
        return pl.ds(pl.multiple_of(k * width, width), width)

    def rows(start, extent):
        return pl.ds(pl.multiple_of(start, size), extent)

    spans = ((size, body), (0, size), (top, size))

    def landing(kind, k):
        start, extent = spans[kind]
        return field.at[pl.ds(start, extent), columns(k)]

    def leaving(kind, d):
        start, extent = ((d * body, body), (d * body - size, size), (d * body + body, size))[kind]
        return basis.at[rows(start, extent), :]

    def to_peer(step, kind):
        d = lax.rem(c + step, nc)
        return remote(leaving(kind, d), landing(kind, c), fsend.at[kind, step], frecv.at[kind, c], cols=d)

    def own(kind):
        return pltpu.make_async_copy(leaving(kind, c), landing(kind, c), lsem.at[kind])

    def down():
        return remote(
            basis.at[pl.ds(nc * body - size, size), :], landing(1, c), fsend.at[1, 0], frecv.at[1, c],
            rows=r + 1, cols=0,
        )

    def up():
        return remote(
            basis.at[pl.ds(0, size), :], landing(2, c), fsend.at[2, 0], frecv.at[2, c],
            rows=r - 1, cols=nc - 1,
        )

    pl.when(r < nr - 1)(lambda: down().start())
    pl.when(r > 0)(lambda: up().start())
    for step in range(1, nc):
        d = lax.rem(c + step, nc)
        to_peer(step, 0).start()
        pl.when(d > 0)(lambda: to_peer(step, 1).start())
        pl.when(d < nc - 1)(lambda: to_peer(step, 2).start())
    own(0).start()
    pl.when(c > 0)(lambda: own(1).start())
    pl.when(c < nc - 1)(lambda: own(2).start())

    @pl.when((r == 0) & (c == 0))
    def _():
        field[0:size, :] = jnp.zeros((size, field.shape[1]), field.dtype)
        wext[0:size, :] = jnp.zeros((size, field.shape[1]), field.dtype)

    @pl.when((r == nr - 1) & (c == nc - 1))
    def _():
        field[top:top + size, :] = jnp.zeros((size, field.shape[1]), field.dtype)
        wext[top:top + size, :] = jnp.zeros((size, field.shape[1]), field.dtype)

    total[...] = jnp.zeros_like(total)

    def arrive(kind, k):
        start, extent = spans[kind]
        remote(
            basis.at[pl.ds(0, extent), :], landing(kind, k), fsend.at[kind, 0], frecv.at[kind, k], cols=k
        ).wait_recv()

    for copy in weights:
        copy.wait()
    own(0).wait()
    pl.when(c > 0)(lambda: own(1).wait())
    pl.when(c < nc - 1)(lambda: own(2).wait())
    for k in range(nc):
        pl.when(k != c)(lambda: arrive(0, k))
        pl.when(((c > 0) & (k != c)) | ((c == 0) & (r > 0)))(lambda: arrive(1, k))
        pl.when(((c < nc - 1) & (k != c)) | ((c == nc - 1) & (r < nr - 1)))(lambda: arrive(2, k))

    def block(i, carry):
        w = apply_block(i, size, field, wl, wd, wu, wi)
        wext[rows((i + 1) * size, size), :] = w
        total[...] += inner(w, w)
        return carry

    lax.fori_loop(0, count, block, 0)

    flat = r * nc + c
    last = nr * nc - 1

    def halo(kind):
        start = (body, size)[kind]
        target = (0, top)[kind]
        to = flat + (1, -1)[kind]
        return remote(
            wext.at[pl.ds(start, size), :], wext.at[pl.ds(target, size), :], hsend.at[kind], hrecv.at[kind],
            rows=to // nc, cols=lax.rem(to, nc),
        )

    place = 0
    across = total.shape[0] // LANES
    for i in range(across):
        for j in range(i, across):
            packed[place * LANES:(place + 1) * LANES, :] = total[
                i * LANES:(i + 1) * LANES, j * LANES:(j + 1) * LANES
            ]
            place += 1
    spare = packed.shape[0] - place * LANES
    if spare:
        packed[place * LANES:, :] = jnp.zeros((spare, LANES), jnp.float32)

    def tile(ref, start, extent):
        return ref.at[pl.ds(pl.multiple_of(start, 8), extent), :]

    finish = exchange(
        "cols", nc, c, lambda d: tile(packed, d * share, share), lambda k: got1.at[k],
        lambda k: got1.at[k], s1, r1,
    )
    pl.when(flat < last)(lambda: halo(0).start())
    pl.when(flat > 0)(lambda: halo(1).start())
    got1[c] = packed[pl.ds(pl.multiple_of(c * share, 8), share), :]
    finish()
    part[...] = sum((got1[k] for k in range(1, nc)), got1[0])
    finish = exchange(
        "rows", nr, r, lambda d: tile(part, d * piece, piece), lambda k: got2.at[k],
        lambda k: got2.at[k], s2, r2,
    )
    got2[r] = part[pl.ds(pl.multiple_of(r * piece, 8), piece), :]
    finish()
    mine = c * share + r * piece
    gram[pl.ds(pl.multiple_of(mine, 8), piece), :] = sum((got2[k] for k in range(1, nr)), got2[0])
    exchange(
        "rows", nr, r, lambda d: tile(gram, mine, piece), lambda k: tile(gram, mine, piece),
        lambda k: tile(gram, c * share + k * piece, piece), s3, r3,
    )()
    exchange(
        "cols", nc, c, lambda d: tile(gram, c * share, share), lambda k: tile(gram, c * share, share),
        lambda k: tile(gram, k * share, share), s4, r4,
    )()

    pl.when(flat < last)(lambda: halo(0).wait_send())
    pl.when(flat > 0)(lambda: halo(1).wait_send())
    pl.when(flat > 0)(lambda: halo(0).wait_recv())
    pl.when(flat < last)(lambda: halo(1).wait_recv())
    pl.when(r < nr - 1)(lambda: down().wait_send())
    pl.when(r > 0)(lambda: up().wait_send())
    for step in range(1, nc):
        d = lax.rem(c + step, nc)
        to_peer(step, 0).wait_send()
        pl.when(d > 0)(lambda: to_peer(step, 1).wait_send())
        pl.when(d < nc - 1)(lambda: to_peer(step, 2).wait_send())


def back_kernel(
    nr, nc, wext, rinv, lower, diag, upper, inverse, ortho, projected,
    oext, wl, wd, wu, wi, total, got1, part, got2,
    wsem, lsem, osend, orecv, s1, r1, s2, r2, s3, r3,
):
    r, c = lax.axis_index("rows"), lax.axis_index("cols")
    count, size, _ = wl.shape
    width = ortho.shape[1]
    body = count * size
    piece = got2.shape[1]

    weights = fetch_blocks((lower, diag, upper, inverse), (wl, wd, wu, wi), wsem, c)

    def at(i):
        return pl.ds(pl.multiple_of(i * size, size), size)

    def turn(i, carry):
        oext[at(i), :] = dot(wext[at(i), :], rinv[...]).astype(jnp.bfloat16)
        return carry

    lax.fori_loop(0, count + 2, turn, 0)

    def columns(k):
        return oext.at[pl.ds(size, body), pl.ds(pl.multiple_of(k * width, width), width)]

    def home(k):
        return ortho.at[pl.ds(pl.multiple_of(k * body, size), body), :]

    finish_ortho = exchange("cols", nc, c, columns, home, home, osend, orecv)
    own = pltpu.make_async_copy(columns(c), home(c), lsem)
    own.start()
    total[...] = jnp.zeros_like(total)
    for copy in weights:
        copy.wait()

    def block(i, carry):
        image = apply_block(i, size, oext, wl, wd, wu, wi)
        total[...] += inner(oext[at(i + 1), :], image)
        return carry

    lax.fori_loop(0, count, block, 0)

    def slab(k):
        return pl.ds(pl.multiple_of(k * width, width), width)

    finish = exchange(
        "cols", nc, c, lambda d: total.at[:, slab(d)], lambda k: got1.at[k], lambda k: got1.at[k], s1, r1
    )
    got1[c] = total[:, slab(c)]
    finish()
    part[...] = sum((got1[k] for k in range(1, nc)), got1[0])

    def tile(ref, k):
        return ref.at[pl.ds(pl.multiple_of(k * piece, 8), piece), :]

    finish = exchange(
        "rows", nr, r, lambda d: tile(part, d), lambda k: got2.at[k], lambda k: got2.at[k], s2, r2
    )
    got2[r] = part[pl.ds(pl.multiple_of(r * piece, 8), piece), :]
    finish()
    projected[pl.ds(pl.multiple_of(r * piece, 8), piece), :] = sum(
        (got2[k] for k in range(1, nr)), got2[0]
    )
    exchange(
        "rows", nr, r, lambda d: tile(projected, r), lambda k: tile(projected, r),
        lambda k: tile(projected, k), s3, r3,
    )()
    own.wait()
    finish_ortho()


def shards(nr, nc, basis, lower, diag, upper, inverse):
    blocks, size, _ = diag.shape
    width = basis.shape[1]
    order = width * nc
    count = blocks // nc
    across = order // LANES
    tiles = across * (across + 1) // 2 * LANES // 8
    piece = -(-tiles // (nr * nc)) * 8
    share = piece * nr
    dma = pltpu.SemaphoreType.DMA
    held = [pltpu.VMEM((count, size, size), jnp.bfloat16)] * 4
    extended = ((count + 2) * size, order)
    pair = lambda n: [dma((n,)), dma((n,))]
    opflops = 8 * count * size * size * order + 2 * count * size * order * order

    wext, gram = pl.pallas_call(
        functools.partial(front_kernel, nr, nc),
        out_shape=(
            jax.ShapeDtypeStruct(extended, jnp.bfloat16),
            jax.ShapeDtypeStruct((nc * share, LANES), jnp.float32),
        ),
        in_specs=[ANY] * 5,
        out_specs=(VMEM, VMEM),
        scratch_shapes=[pltpu.VMEM(extended, jnp.bfloat16)] + held + [
            pltpu.VMEM((order, order), jnp.float32),
            pltpu.VMEM((nc * share, LANES), jnp.float32),
            pltpu.VMEM((nc, share, LANES), jnp.float32),
            pltpu.VMEM((share, LANES), jnp.float32),
            pltpu.VMEM((nr, piece, LANES), jnp.float32),
            dma((4,)), dma((3,)), dma((3, nc)), dma((3, nc)), dma((2,)), dma((2,)),
        ] + pair(nc) + pair(nr) + pair(nr) + pair(nc),
        compiler_params=pltpu.CompilerParams(has_side_effects=True),
        cost_estimate=pl.CostEstimate(flops=opflops, bytes_accessed=1 << 23, transcendentals=0),
        name="front",
    )(basis, lower, diag, upper, inverse)

    rinv = inverse_upper(gram, order)

    lines = order // nr
    return pl.pallas_call(
        functools.partial(back_kernel, nr, nc),
        out_shape=(
            jax.ShapeDtypeStruct(basis.shape, jnp.bfloat16),
            jax.ShapeDtypeStruct((order, width), jnp.float32),
        ),
        in_specs=[VMEM, VMEM] + [ANY] * 4,
        out_specs=(ANY, VMEM),
        scratch_shapes=[pltpu.VMEM(extended, jnp.bfloat16)] + held + [
            pltpu.VMEM((order, order), jnp.float32),
            pltpu.VMEM((nc, order, width), jnp.float32),
            pltpu.VMEM((order, width), jnp.float32),
            pltpu.VMEM((nr, lines, width), jnp.float32),
            dma((4,)), dma,
        ] + pair(nc) + pair(nc) + pair(nr) + pair(nr),
        compiler_params=pltpu.CompilerParams(has_side_effects=True),
        cost_estimate=pl.CostEstimate(flops=opflops, bytes_accessed=1 << 23, transcendentals=0),
        name="back",
    )(wext, rinv, lower, diag, upper, inverse)


def solution(mesh):
    in_specs = (
        P("rows", "cols"),
        P("rows", None, None),
        P("rows", None, None),
        P("rows", None, None),
        P("rows", None, None),
    )
    out_specs = (P("rows", "cols"), P(None, "cols"))
    body = functools.partial(shards, mesh.shape["rows"], mesh.shape["cols"])
    return jax.shard_map(body, mesh=mesh, in_specs=in_specs, out_specs=out_specs, check_vma=False)
```

```python
import functools

import jax
import jax.numpy as jnp
from jax import lax
from jax.experimental import pallas as pl
from jax.experimental.pallas import tpu as pltpu
from jax.sharding import PartitionSpec as P

LANES = 128
CHUNK = 2
MESH = pl.DeviceIdType.MESH
VMEM = pl.BlockSpec(memory_space=pltpu.VMEM)
ANY = pl.BlockSpec(memory_space=pl.ANY)
SUB = 8
HI = lax.Precision.HIGHEST

def factor_tile(block):
    size = block.shape[0]
    wide = (SUB, size)
    tiles = size // SUB
    row_of = lax.broadcasted_iota(jnp.int32, wide, 0)
    lane_of = lax.broadcasted_iota(jnp.int32, wide, 1)
    a = [block[t * SUB:(t + 1) * SUB, :] for t in range(tiles)]
    m = [jnp.where(lane_of == row_of + t * SUB, 1.0, 0.0).astype(jnp.float32) for t in range(tiles)]
    out = []
    for t in range(tiles):
        at, mt = a[t], m[t]
        base = t * SUB
        pivot = {}
        for i in range(SUB):
            for j in range(i + 1):
                pivot[i, j] = jnp.broadcast_to(at[i:i + 1, base + j:base + j + 1], wide)
        ra = [jnp.broadcast_to(at[i:i + 1, :], wide) for i in range(SUB)]
        rm = [jnp.broadcast_to(mt[i:i + 1, :], wide) for i in range(SUB)]
        last = t == tiles - 1
        unit = {}
        sa, sm = [None] * SUB, [None] * SUB
        fin = jnp.zeros(wide, jnp.float32)
        for j in range(SUB):
            d = pivot[j, j]
            root = lax.rsqrt(d)
            inv = 1.0 / d
            fin = jnp.where(row_of == j, rm[j] * root, fin)
            for i in range(j + 1, SUB):
                unit[i, j] = pivot[i, j] * inv
            for i in range(j + 1, SUB):
                for q in range(j + 1, i + 1):
                    pivot[i, q] = pivot[i, q] - unit[i, j] * pivot[q, j]
            for i in range(j + 1, SUB):
                if not last:
                    ra[i] = ra[i] - unit[i, j] * ra[j]
                rm[i] = rm[i] - unit[i, j] * rm[j]
            if not last:
                sa[j] = ra[j] * inv
                sm[j] = rm[j] * inv
        out.append(fin)
        if last:
            break
        for j in range(SUB - 1, -1, -1):
            for i in range(j):
                sa[i] = sa[i] - unit[j, i] * sa[j]
                sm[i] = sm[i] - unit[j, i] * sm[j]
        for s in range(t + 1, tiles):
            na, nm = a[s], m[s]
            for j in range(SUB):
                c = jnp.broadcast_to(a[s][:, base + j:base + j + 1], wide)
                na = na - c * sa[j]
                nm = nm - c * sm[j]
            a[s], m[s] = na, nm
    return jnp.concatenate(out, axis=0)

def inverse_upper_steps(work_ref, out_ref, panel_ref):
    n, size, _ = work_ref.shape
    order = n * size
    def step(b, carry):
        at = [work_ref[b, :, i * size:(i + 1) * size] for i in range(n)]
        block = at[0]
        for i in range(1, n):
            block = jnp.where(b == i, at[i], block)
        linv = factor_tile(block)
        y = lax.dot_general(linv, work_ref[b], (((1,), (0,)), ((), ())), precision=HI, preferred_element_type=jnp.float32)
        work_ref[b] = y
        for i in range(n):
            panel_ref[i] = y[:, i * size:(i + 1) * size]
        def below(i, c):
            work_ref[i] = work_ref[i] - lax.dot_general(panel_ref[i], y_ref[...], (((0,), (0,)), ((), ())), precision=HI, preferred_element_type=jnp.float32)
            return c
        y_ref = work_ref.at[b]
        lax.fori_loop(b + 1, n, below, 0)
        return carry
    lax.fori_loop(0, n, step, 0)
    for b in range(n):
        out_ref[:, b * size:(b + 1) * size] = work_ref[b, :, order:].T.astype(out_ref.dtype)

def unpack_kernel(packed_ref, out_ref, work_ref, panel_ref):
    n, size, _ = work_ref.shape
    order = n * size
    row = lax.broadcasted_iota(jnp.int32, (size, order), 0)
    lane = lax.broadcasted_iota(jnp.int32, (size, order), 1)
    place = 0
    for i in range(n):
        work_ref[i, :, :order] = jnp.zeros((size, order), jnp.float32)
        work_ref[i, :, order:] = jnp.where(lane == row + i * size, 1.0, 0.0).astype(jnp.float32)
        for j in range(i, n):
            work_ref[i, :, j * size:(j + 1) * size] = packed_ref[place * size:(place + 1) * size, :]
            place += 1
    inverse_upper_steps(work_ref, out_ref, panel_ref)


def inverse_upper(packed, order):
    n = order // LANES
    return pl.pallas_call(
        unpack_kernel,
        out_shape=jax.ShapeDtypeStruct((order, order), jnp.bfloat16),
        in_specs=[VMEM],
        out_specs=VMEM,
        scratch_shapes=[
            pltpu.VMEM((n, LANES, 2 * order), jnp.float32),
            pltpu.VMEM((n, LANES, LANES), jnp.float32),
        ],
        cost_estimate=pl.CostEstimate(
            flops=8 * order**3, bytes_accessed=8 * order * order, transcendentals=0
        ),
        name="inverse_upper",
    )(packed)


def dot(left, right):
    return jnp.dot(left, right, preferred_element_type=jnp.float32)


def inner(left, right):
    return lax.dot_general(
        left, right, (((0,), (0,)), ((), ())), preferred_element_type=jnp.float32
    )


def remote(src, dst, send, recv, **where):
    return pltpu.make_async_remote_copy(
        src_ref=src, dst_ref=dst, send_sem=send, recv_sem=recv, device_id=where, device_id_type=MESH
    )


def exchange(axis, count, me, source, target, arrived, send, recv):
    for step in range(1, count):
        peer = lax.rem(me + step, count)
        remote(source(peer), target(me), send.at[step], recv.at[me], **{axis: peer}).start()

    def finish():
        for step in range(1, count):
            peer = lax.rem(me + step, count)
            remote(
                source(peer), arrived(peer), send.at[step], recv.at[peer], **{axis: peer}
            ).wait()

    return finish


def flip(index, bit):
    return index + bit - 2 * bit * lax.rem(index // bit, 2)


def flips(index, mask):
    bit = 1
    while bit <= mask:
        if mask & bit:
            index = flip(index, bit)
        bit *= 2
    return index


def apply_block(i, size, field, wl, wd, wu, wi):
    def at(k):
        return field[pl.ds(pl.multiple_of(k * size, size), size), :]

    mixed = dot(wl[i], at(i)) + dot(wd[i], at(i + 1)) + dot(wu[i], at(i + 2))
    return dot(wi[i], mixed.astype(jnp.bfloat16)).astype(jnp.bfloat16)


def fetch_blocks(parts, held, sem, first):
    count = held[0].shape[0]
    copies = [
        pltpu.make_async_copy(part.at[pl.ds(first * count, count)], ref, sem.at[k])
        for k, (part, ref) in enumerate(zip(parts, held))
    ]
    for copy in copies:
        copy.start()
    return copies


def front_kernel(
    nr, nc, basis, lower, diag, upper, inverse, wext, gram,
    field, wl, wd, wu, wi, total, packed, got1, part, got2,
    wsem, lsem, fsend, frecv, hsend, hrecv, s1, r1, s2, r2, s3, r3, s4, r4,
):
    r, c = lax.axis_index("rows"), lax.axis_index("cols")
    count, size, _ = wl.shape
    width = basis.shape[1]
    body = count * size
    top = (count + 1) * size
    share = got1.shape[1]
    piece = got2.shape[1]

    weights = fetch_blocks((lower, diag, upper, inverse), (wl, wd, wu, wi), wsem, c)

    def columns(k):
        return pl.ds(pl.multiple_of(k * width, width), width)

    def rows(start, extent):
        return pl.ds(pl.multiple_of(start, size), extent)

    group = CHUNK * size
    lump = body // group
    high = lump + 1
    spans = [(0, size)] + [(size + k * group, group) for k in range(lump)] + [(top, size)]

    def landing(kind, k):
        start, extent = spans[kind]
        return field.at[pl.ds(start, extent), columns(k)]

    def leaving(kind, d):
        start, extent = spans[kind]
        return basis.at[rows(d * body - size + start, extent), :]

    def to_peer(step, kind):
        d = lax.rem(c + step, nc)
        return remote(leaving(kind, d), landing(kind, c), fsend.at[kind, step], frecv.at[kind, c], cols=d)

    def own(kind):
        return pltpu.make_async_copy(leaving(kind, c), landing(kind, c), lsem.at[kind])

    def down():
        return remote(
            basis.at[pl.ds(nc * body - size, size), :], landing(0, c), fsend.at[0, 0], frecv.at[0, c],
            rows=r + 1, cols=0,
        )

    def up():
        return remote(
            basis.at[pl.ds(0, size), :], landing(high, c), fsend.at[high, 0], frecv.at[high, c],
            rows=r - 1, cols=nc - 1,
        )

    def each(kind, action):
        for step in range(1, nc):
            d = lax.rem(c + step, nc)
            send = functools.partial(action, step, kind)
            if kind == 0:
                pl.when(d > 0)(send)
            elif kind == high:
                pl.when(d < nc - 1)(send)
            else:
                send()

    def mine_too(kind, action):
        if kind == 0:
            pl.when(c > 0)(action)
        elif kind == high:
            pl.when(c < nc - 1)(action)
        else:
            action()

    pl.when(r < nr - 1)(lambda: down().start())
    for kind in range(high + 1):
        mine_too(kind, lambda: own(kind).start())
        each(kind, lambda step, kind: to_peer(step, kind).start())
        if kind == 1:
            pl.when(r > 0)(lambda: up().start())

    @pl.when((r == 0) & (c == 0))
    def _():
        field[0:size, :] = jnp.zeros((size, field.shape[1]), field.dtype)
        wext[0:size, :] = jnp.zeros((size, field.shape[1]), field.dtype)

    @pl.when((r == nr - 1) & (c == nc - 1))
    def _():
        field[top:top + size, :] = jnp.zeros((size, field.shape[1]), field.dtype)
        wext[top:top + size, :] = jnp.zeros((size, field.shape[1]), field.dtype)

    total[...] = jnp.zeros_like(total)

    def arrive(kind, k):
        start, extent = spans[kind]
        remote(
            basis.at[pl.ds(0, extent), :], landing(kind, k), fsend.at[kind, 0], frecv.at[kind, k], cols=k
        ).wait_recv()

    def block(i, carry):
        w = apply_block(i, size, field, wl, wd, wu, wi)
        wext[rows((i + 1) * size, size), :] = w
        total[...] += inner(w, w)
        return carry

    for copy in weights:
        copy.wait()
    done = 0
    for kind in range(high + 1):
        mine_too(kind, lambda: own(kind).wait())
        for k in range(nc):
            comes = k != c
            if kind == 0:
                comes = ((c > 0) & comes) | ((c == 0) & (r > 0))
            elif kind == high:
                comes = ((c < nc - 1) & comes) | ((c == nc - 1) & (r < nr - 1))
            pl.when(comes)(lambda: arrive(kind, k))
        ready = count if kind == high else max(kind * CHUNK - 1, 0)
        if ready > done:
            lax.fori_loop(done, ready, block, 0)
            done = ready

    flat = r * nc + c
    last = nr * nc - 1

    def halo(kind):
        start = (body, size)[kind]
        target = (0, top)[kind]
        to = flat + (1, -1)[kind]
        return remote(
            wext.at[pl.ds(start, size), :], wext.at[pl.ds(target, size), :], hsend.at[kind], hrecv.at[kind],
            rows=to // nc, cols=lax.rem(to, nc),
        )

    place = 0
    across = total.shape[0] // LANES
    for i in range(across):
        for j in range(i, across):
            packed[place * LANES:(place + 1) * LANES, :] = total[
                i * LANES:(i + 1) * LANES, j * LANES:(j + 1) * LANES
            ]
            place += 1
    spare = packed.shape[0] - place * LANES
    if spare:
        packed[place * LANES:, :] = jnp.zeros((spare, LANES), jnp.float32)

    def tile(ref, start, extent):
        return ref.at[pl.ds(pl.multiple_of(start, 8), extent), :]

    finish = exchange(
        "cols", nc, c, lambda d: tile(packed, d * share, share), lambda k: got1.at[k],
        lambda k: got1.at[k], s1, r1,
    )
    got1[c] = packed[pl.ds(pl.multiple_of(c * share, 8), share), :]
    finish()
    pl.when(flat < last)(lambda: halo(0).start())
    pl.when(flat > 0)(lambda: halo(1).start())
    part[...] = sum((got1[k] for k in range(1, nc)), got1[0])
    finish = exchange(
        "rows", nr, r, lambda d: tile(part, d * piece, piece), lambda k: got2.at[k],
        lambda k: got2.at[k], s2, r2,
    )
    got2[r] = part[pl.ds(pl.multiple_of(r * piece, 8), piece), :]
    finish()
    mine = c * share + r * piece
    gram[pl.ds(pl.multiple_of(mine, 8), piece), :] = sum((got2[k] for k in range(1, nr)), got2[0])
    exchange(
        "rows", nr, r, lambda d: tile(gram, mine, piece), lambda k: tile(gram, mine, piece),
        lambda k: tile(gram, c * share + k * piece, piece), s3, r3,
    )()
    exchange(
        "cols", nc, c, lambda d: tile(gram, c * share, share), lambda k: tile(gram, c * share, share),
        lambda k: tile(gram, k * share, share), s4, r4,
    )()

    pl.when(flat < last)(lambda: halo(0).wait_send())
    pl.when(flat > 0)(lambda: halo(1).wait_send())
    pl.when(flat > 0)(lambda: halo(0).wait_recv())
    pl.when(flat < last)(lambda: halo(1).wait_recv())
    pl.when(r < nr - 1)(lambda: down().wait_send())
    pl.when(r > 0)(lambda: up().wait_send())
    for kind in range(high + 1):
        each(kind, lambda step, kind: to_peer(step, kind).wait_send())


def back_kernel(
    nr, nc, wext, rinv, lower, diag, upper, inverse, ortho, projected,
    oext, wl, wd, wu, wi, total, got1, part, got2,
    wsem, lsem, osend, orecv, esend, erecv, s1, r1, s2, r2, s3, r3,
):
    r, c = lax.axis_index("rows"), lax.axis_index("cols")
    count, size, _ = wl.shape
    width = ortho.shape[1]
    body = count * size
    piece = got2.shape[1]

    weights = fetch_blocks((lower, diag, upper, inverse), (wl, wd, wu, wi), wsem, c)

    def at(i):
        return pl.ds(pl.multiple_of(i * size, size), size)

    def turn(i, carry):
        oext[at(i), :] = dot(wext[at(i), :], rinv[...]).astype(jnp.bfloat16)
        return carry

    lax.fori_loop(0, count + 2, turn, 0)

    early = (count // 2) * size

    def columns(start, extent, k):
        return oext.at[pl.ds(size + start, extent), pl.ds(pl.multiple_of(k * width, width), width)]

    def home(start, extent, k):
        return ortho.at[pl.ds(pl.multiple_of(k * body + start, size), extent), :]

    def go_home(start, extent, send, recv):
        there = functools.partial(home, start, extent)
        return exchange(
            "cols", nc, c, functools.partial(columns, start, extent), there, there, send, recv
        )

    finish_early = go_home(0, early, osend, orecv)
    own = pltpu.make_async_copy(columns(0, body, c), home(0, body, c), lsem)
    own.start()
    total[...] = jnp.zeros_like(total)
    for copy in weights:
        copy.wait()

    def block(i, carry):
        image = apply_block(i, size, oext, wl, wd, wu, wi)
        total[...] += inner(oext[at(i + 1), :], image)
        return carry

    lax.fori_loop(0, count, block, 0)

    def slab(k):
        return pl.ds(pl.multiple_of(k * width, width), width)

    bit, used = 1, 0
    kept = list(range(0, nc))
    while bit < nc:
        peer = flip(c, bit)
        kept = [k for k in kept if k & bit == 0]
        copies = [
            remote(
                total.at[:, slab(flips(peer, k))], got1.at[used + n], s1.at[used + n], r1.at[used + n],
                cols=peer,
            )
            for n, k in enumerate(kept)
        ]
        for copy in copies:
            copy.start()
        if 2 * bit == nc:
            finish_late = go_home(early, body - early, esend, erecv)
        for n, (k, copy) in enumerate(zip(kept, copies)):
            copy.wait()
            where = slab(flips(c, k))
            if 2 * bit == nc:
                part[...] = total[:, where] + got1[used + n]
            else:
                total[:, where] = total[:, where] + got1[used + n]
        used += len(kept)
        bit *= 2

    def tile(ref, k):
        return ref.at[pl.ds(pl.multiple_of(k * piece, 8), piece), :]

    finish = exchange(
        "rows", nr, r, lambda d: tile(part, d), lambda k: got2.at[k], lambda k: got2.at[k], s2, r2
    )
    got2[r] = part[pl.ds(pl.multiple_of(r * piece, 8), piece), :]
    finish()
    projected[pl.ds(pl.multiple_of(r * piece, 8), piece), :] = sum(
        (got2[k] for k in range(1, nr)), got2[0]
    )
    exchange(
        "rows", nr, r, lambda d: tile(projected, r), lambda k: tile(projected, r),
        lambda k: tile(projected, k), s3, r3,
    )()
    own.wait()
    finish_early()
    finish_late()


def shards(nr, nc, basis, lower, diag, upper, inverse):
    blocks, size, _ = diag.shape
    width = basis.shape[1]
    order = width * nc
    count = blocks // nc
    across = order // LANES
    tiles = across * (across + 1) // 2 * LANES // 8
    piece = -(-tiles // (nr * nc)) * 8
    share = piece * nr
    dma = pltpu.SemaphoreType.DMA
    held = [pltpu.VMEM((count, size, size), jnp.bfloat16)] * 4
    extended = ((count + 2) * size, order)
    pair = lambda n: [dma((n,)), dma((n,))]
    kinds = count // CHUNK + 2
    opflops = 8 * count * size * size * order + 2 * count * size * order * order

    wext, gram = pl.pallas_call(
        functools.partial(front_kernel, nr, nc),
        out_shape=(
            jax.ShapeDtypeStruct(extended, jnp.bfloat16),
            jax.ShapeDtypeStruct((nc * share, LANES), jnp.float32),
        ),
        in_specs=[ANY] * 5,
        out_specs=(VMEM, VMEM),
        scratch_shapes=[pltpu.VMEM(extended, jnp.bfloat16)] + held + [
            pltpu.VMEM((order, order), jnp.float32),
            pltpu.VMEM((nc * share, LANES), jnp.float32),
            pltpu.VMEM((nc, share, LANES), jnp.float32),
            pltpu.VMEM((share, LANES), jnp.float32),
            pltpu.VMEM((nr, piece, LANES), jnp.float32),
            dma((4,)), dma((kinds,)), dma((kinds, nc)), dma((kinds, nc)), dma((2,)), dma((2,)),
        ] + pair(nc) + pair(nr) + pair(nr) + pair(nc),
        compiler_params=pltpu.CompilerParams(has_side_effects=True),
        cost_estimate=pl.CostEstimate(flops=opflops, bytes_accessed=1 << 23, transcendentals=0),
        name="front",
    )(basis, lower, diag, upper, inverse)

    rinv = inverse_upper(gram, order)

    lines = order // nr
    return pl.pallas_call(
        functools.partial(back_kernel, nr, nc),
        out_shape=(
            jax.ShapeDtypeStruct(basis.shape, jnp.bfloat16),
            jax.ShapeDtypeStruct((order, width), jnp.float32),
        ),
        in_specs=[VMEM, VMEM] + [ANY] * 4,
        out_specs=(ANY, VMEM),
        scratch_shapes=[pltpu.VMEM(extended, jnp.bfloat16)] + held + [
            pltpu.VMEM((order, order), jnp.float32),
            pltpu.VMEM((nc, order, width), jnp.float32),
            pltpu.VMEM((order, width), jnp.float32),
            pltpu.VMEM((nr, lines, width), jnp.float32),
            dma((4,)), dma,
        ] + pair(nc) + pair(nc) + pair(nc) + pair(nr) + pair(nr),
        compiler_params=pltpu.CompilerParams(has_side_effects=True),
        cost_estimate=pl.CostEstimate(flops=opflops, bytes_accessed=1 << 23, transcendentals=0),
        name="back",
    )(wext, rinv, lower, diag, upper, inverse)


def solution(mesh):
    in_specs = (
        P("rows", "cols"),
        P("rows", None, None),
        P("rows", None, None),
        P("rows", None, None),
        P("rows", None, None),
    )
    out_specs = (P("rows", "cols"), P(None, "cols"))
    body = functools.partial(shards, mesh.shape["rows"], mesh.shape["cols"])
    return jax.shard_map(body, mesh=mesh, in_specs=in_specs, out_specs=out_specs, check_vma=False)
```

```python
import functools

import jax
import jax.numpy as jnp
from jax import lax
from jax.experimental import pallas as pl
from jax.experimental.pallas import tpu as pltpu
from jax.sharding import PartitionSpec as P

LANES = 128
CHUNK = 2
MESH = pl.DeviceIdType.MESH
VMEM = pl.BlockSpec(memory_space=pltpu.VMEM)
ANY = pl.BlockSpec(memory_space=pl.ANY)
SUB = 8
HI = lax.Precision.HIGHEST

def factor_tile(block):
    size = block.shape[0]
    wide = (SUB, size)
    tiles = size // SUB
    row_of = lax.broadcasted_iota(jnp.int32, wide, 0)
    lane_of = lax.broadcasted_iota(jnp.int32, wide, 1)
    a = [block[t * SUB:(t + 1) * SUB, :] for t in range(tiles)]
    m = [jnp.where(lane_of == row_of + t * SUB, 1.0, 0.0).astype(jnp.float32) for t in range(tiles)]
    out = []
    for t in range(tiles):
        at, mt = a[t], m[t]
        base = t * SUB
        pivot = {}
        for i in range(SUB):
            for j in range(i + 1):
                pivot[i, j] = jnp.broadcast_to(at[i:i + 1, base + j:base + j + 1], wide)
        ra = [jnp.broadcast_to(at[i:i + 1, :], wide) for i in range(SUB)]
        rm = [jnp.broadcast_to(mt[i:i + 1, :], wide) for i in range(SUB)]
        last = t == tiles - 1
        unit = {}
        sa, sm = [None] * SUB, [None] * SUB
        fin = jnp.zeros(wide, jnp.float32)
        for j in range(SUB):
            d = pivot[j, j]
            root = lax.rsqrt(d)
            inv = 1.0 / d
            fin = jnp.where(row_of == j, rm[j] * root, fin)
            for i in range(j + 1, SUB):
                unit[i, j] = pivot[i, j] * inv
            for i in range(j + 1, SUB):
                for q in range(j + 1, i + 1):
                    pivot[i, q] = pivot[i, q] - unit[i, j] * pivot[q, j]
            for i in range(j + 1, SUB):
                if not last:
                    ra[i] = ra[i] - unit[i, j] * ra[j]
                rm[i] = rm[i] - unit[i, j] * rm[j]
            if not last:
                sa[j] = ra[j] * inv
                sm[j] = rm[j] * inv
        out.append(fin)
        if last:
            break
        for j in range(SUB - 1, -1, -1):
            for i in range(j):
                sa[i] = sa[i] - unit[j, i] * sa[j]
                sm[i] = sm[i] - unit[j, i] * sm[j]
        for s in range(t + 1, tiles):
            na, nm = a[s], m[s]
            for j in range(SUB):
                c = jnp.broadcast_to(a[s][:, base + j:base + j + 1], wide)
                na = na - c * sa[j]
                nm = nm - c * sm[j]
            a[s], m[s] = na, nm
    return jnp.concatenate(out, axis=0)

def inverse_upper_steps(work_ref, out_ref, panel_ref):
    n, size, _ = work_ref.shape
    order = n * size
    def step(b, carry):
        at = [work_ref[b, :, i * size:(i + 1) * size] for i in range(n)]
        block = at[0]
        for i in range(1, n):
            block = jnp.where(b == i, at[i], block)
        linv = factor_tile(block)
        live = pl.ds(pl.multiple_of(b * size, size), order + size)
        work_ref[b, :, live] = lax.dot_general(
            linv, work_ref[b, :, live], (((1,), (0,)), ((), ())), precision=HI,
            preferred_element_type=jnp.float32,
        )
        for i in range(n):
            panel_ref[i] = work_ref[b, :, i * size:(i + 1) * size]

        def below(i, c):
            work_ref[i, :, live] = work_ref[i, :, live] - lax.dot_general(
                panel_ref[i], work_ref[b, :, live], (((0,), (0,)), ((), ())), precision=HI,
                preferred_element_type=jnp.float32,
            )
            return c

        lax.fori_loop(b + 1, n, below, 0)
        return carry
    lax.fori_loop(0, n, step, 0)
    for b in range(n):
        out_ref[:, b * size:(b + 1) * size] = work_ref[b, :, order:].T.astype(out_ref.dtype)

def unpack_kernel(packed_ref, out_ref, work_ref, panel_ref):
    n, size, _ = work_ref.shape
    order = n * size
    row = lax.broadcasted_iota(jnp.int32, (size, order), 0)
    lane = lax.broadcasted_iota(jnp.int32, (size, order), 1)
    place = 0
    for i in range(n):
        work_ref[i, :, :order] = jnp.zeros((size, order), jnp.float32)
        work_ref[i, :, order:] = jnp.where(lane == row + i * size, 1.0, 0.0).astype(jnp.float32)
        for j in range(i, n):
            work_ref[i, :, j * size:(j + 1) * size] = packed_ref[place * size:(place + 1) * size, :]
            place += 1
    inverse_upper_steps(work_ref, out_ref, panel_ref)


def inverse_upper(packed, order):
    n = order // LANES
    return pl.pallas_call(
        unpack_kernel,
        out_shape=jax.ShapeDtypeStruct((order, order), jnp.bfloat16),
        in_specs=[VMEM],
        out_specs=VMEM,
        scratch_shapes=[
            pltpu.VMEM((n, LANES, 2 * order), jnp.float32),
            pltpu.VMEM((n, LANES, LANES), jnp.float32),
        ],
        cost_estimate=pl.CostEstimate(
            flops=8 * order**3, bytes_accessed=8 * order * order, transcendentals=0
        ),
        name="inverse_upper",
    )(packed)


def dot(left, right):
    return jnp.dot(left, right, preferred_element_type=jnp.float32)


def inner(left, right):
    return lax.dot_general(
        left, right, (((0,), (0,)), ((), ())), preferred_element_type=jnp.float32
    )


def remote(src, dst, send, recv, **where):
    return pltpu.make_async_remote_copy(
        src_ref=src, dst_ref=dst, send_sem=send, recv_sem=recv, device_id=where, device_id_type=MESH
    )


def exchange(axis, count, me, source, target, arrived, send, recv):
    for step in range(1, count):
        peer = lax.rem(me + step, count)
        remote(source(peer), target(me), send.at[step], recv.at[me], **{axis: peer}).start()

    def finish():
        for step in range(1, count):
            peer = lax.rem(me + step, count)
            remote(
                source(peer), arrived(peer), send.at[step], recv.at[peer], **{axis: peer}
            ).wait()

    return finish


def flip(index, bit):
    return index + bit - 2 * bit * lax.rem(index // bit, 2)


def flips(index, mask):
    bit = 1
    while bit <= mask:
        if mask & bit:
            index = flip(index, bit)
        bit *= 2
    return index


def apply_block(i, size, field, wl, wd, wu, wi):
    def at(k):
        return field[pl.ds(pl.multiple_of(k * size, size), size), :]

    mixed = dot(wl[i], at(i)) + dot(wd[i], at(i + 1)) + dot(wu[i], at(i + 2))
    return dot(wi[i], mixed.astype(jnp.bfloat16)).astype(jnp.bfloat16)


def fetch_blocks(parts, held, sem, first):
    count = held[0].shape[0]
    copies = [
        pltpu.make_async_copy(part.at[pl.ds(first * count, count)], ref, sem.at[k])
        for k, (part, ref) in enumerate(zip(parts, held))
    ]
    for copy in copies:
        copy.start()
    return copies


def front_kernel(
    nr, nc, basis, lower, diag, upper, inverse, wext, gram,
    field, wl, wd, wu, wi, total, packed, got1, part, got2,
    wsem, lsem, fsend, frecv, hsend, hrecv, s1, r1, s2, r2, s3, r3, s4, r4,
):
    r, c = lax.axis_index("rows"), lax.axis_index("cols")
    count, size, _ = wl.shape
    width = basis.shape[1]
    body = count * size
    top = (count + 1) * size
    share = got1.shape[1]
    piece = got2.shape[1]

    weights = fetch_blocks((lower, diag, upper, inverse), (wl, wd, wu, wi), wsem, c)

    def columns(k):
        return pl.ds(pl.multiple_of(k * width, width), width)

    def rows(start, extent):
        return pl.ds(pl.multiple_of(start, size), extent)

    group = CHUNK * size
    lump = body // group
    high = lump + 1
    spans = [(0, size)] + [(size + k * group, group) for k in range(lump)] + [(top, size)]

    def landing(kind, k):
        start, extent = spans[kind]
        return field.at[pl.ds(start, extent), columns(k)]

    def leaving(kind, d):
        start, extent = spans[kind]
        return basis.at[rows(d * body - size + start, extent), :]

    def to_peer(step, kind):
        d = lax.rem(c + step, nc)
        return remote(leaving(kind, d), landing(kind, c), fsend.at[kind, step], frecv.at[kind, c], cols=d)

    def own(kind):
        return pltpu.make_async_copy(leaving(kind, c), landing(kind, c), lsem.at[kind])

    def down():
        return remote(
            basis.at[pl.ds(nc * body - size, size), :], landing(0, c), fsend.at[0, 0], frecv.at[0, c],
            rows=r + 1, cols=0,
        )

    def up():
        return remote(
            basis.at[pl.ds(0, size), :], landing(high, c), fsend.at[high, 0], frecv.at[high, c],
            rows=r - 1, cols=nc - 1,
        )

    def each(kind, action):
        for step in range(1, nc):
            d = lax.rem(c + step, nc)
            send = functools.partial(action, step, kind)
            if kind == 0:
                pl.when(d > 0)(send)
            elif kind == high:
                pl.when(d < nc - 1)(send)
            else:
                send()

    def mine_too(kind, action):
        if kind == 0:
            pl.when(c > 0)(action)
        elif kind == high:
            pl.when(c < nc - 1)(action)
        else:
            action()

    pl.when(r < nr - 1)(lambda: down().start())
    for kind in range(high + 1):
        mine_too(kind, lambda: own(kind).start())
        each(kind, lambda step, kind: to_peer(step, kind).start())
        if kind == 1:
            pl.when(r > 0)(lambda: up().start())

    @pl.when((r == 0) & (c == 0))
    def _():
        field[0:size, :] = jnp.zeros((size, field.shape[1]), field.dtype)
        wext[0:size, :] = jnp.zeros((size, field.shape[1]), field.dtype)

    @pl.when((r == nr - 1) & (c == nc - 1))
    def _():
        field[top:top + size, :] = jnp.zeros((size, field.shape[1]), field.dtype)
        wext[top:top + size, :] = jnp.zeros((size, field.shape[1]), field.dtype)

    total[...] = jnp.zeros_like(total)

    def arrive(kind, k):
        start, extent = spans[kind]
        remote(
            basis.at[pl.ds(0, extent), :], landing(kind, k), fsend.at[kind, 0], frecv.at[kind, k], cols=k
        ).wait_recv()

    def block(i, carry):
        w = apply_block(i, size, field, wl, wd, wu, wi)
        wext[rows((i + 1) * size, size), :] = w
        total[...] += inner(w, w)
        return carry

    for copy in weights:
        copy.wait()
    done = 0
    for kind in range(high + 1):
        mine_too(kind, lambda: own(kind).wait())
        for k in range(nc):
            comes = k != c
            if kind == 0:
                comes = ((c > 0) & comes) | ((c == 0) & (r > 0))
            elif kind == high:
                comes = ((c < nc - 1) & comes) | ((c == nc - 1) & (r < nr - 1))
            pl.when(comes)(lambda: arrive(kind, k))
        ready = count if kind == high else max(kind * CHUNK - 1, 0)
        if ready > done:
            lax.fori_loop(done, ready, block, 0)
            done = ready

    flat = r * nc + c
    last = nr * nc - 1

    def halo(kind):
        start = (body, size)[kind]
        target = (0, top)[kind]
        to = flat + (1, -1)[kind]
        return remote(
            wext.at[pl.ds(start, size), :], wext.at[pl.ds(target, size), :], hsend.at[kind], hrecv.at[kind],
            rows=to // nc, cols=lax.rem(to, nc),
        )

    place = 0
    across = total.shape[0] // LANES
    for i in range(across):
        for j in range(i, across):
            packed[place * LANES:(place + 1) * LANES, :] = total[
                i * LANES:(i + 1) * LANES, j * LANES:(j + 1) * LANES
            ]
            place += 1
    spare = packed.shape[0] - place * LANES
    if spare:
        packed[place * LANES:, :] = jnp.zeros((spare, LANES), jnp.float32)

    def tile(ref, start, extent):
        return ref.at[pl.ds(pl.multiple_of(start, 8), extent), :]

    finish = exchange(
        "cols", nc, c, lambda d: tile(packed, d * share, share), lambda k: got1.at[k],
        lambda k: got1.at[k], s1, r1,
    )
    got1[c] = packed[pl.ds(pl.multiple_of(c * share, 8), share), :]
    finish()
    pl.when(flat < last)(lambda: halo(0).start())
    pl.when(flat > 0)(lambda: halo(1).start())
    part[...] = sum((got1[k] for k in range(1, nc)), got1[0])
    finish = exchange(
        "rows", nr, r, lambda d: tile(part, d * piece, piece), lambda k: got2.at[k],
        lambda k: got2.at[k], s2, r2,
    )
    got2[r] = part[pl.ds(pl.multiple_of(r * piece, 8), piece), :]
    finish()
    mine = c * share + r * piece
    gram[pl.ds(pl.multiple_of(mine, 8), piece), :] = sum((got2[k] for k in range(1, nr)), got2[0])
    exchange(
        "rows", nr, r, lambda d: tile(gram, mine, piece), lambda k: tile(gram, mine, piece),
        lambda k: tile(gram, c * share + k * piece, piece), s3, r3,
    )()
    exchange(
        "cols", nc, c, lambda d: tile(gram, c * share, share), lambda k: tile(gram, c * share, share),
        lambda k: tile(gram, k * share, share), s4, r4,
    )()

    pl.when(flat < last)(lambda: halo(0).wait_send())
    pl.when(flat > 0)(lambda: halo(1).wait_send())
    pl.when(flat > 0)(lambda: halo(0).wait_recv())
    pl.when(flat < last)(lambda: halo(1).wait_recv())
    pl.when(r < nr - 1)(lambda: down().wait_send())
    pl.when(r > 0)(lambda: up().wait_send())
    for kind in range(high + 1):
        each(kind, lambda step, kind: to_peer(step, kind).wait_send())


def back_kernel(
    nr, nc, wext, rinv, lower, diag, upper, inverse, ortho, projected,
    oext, wl, wd, wu, wi, total, got1, part, got2,
    wsem, lsem, osend, orecv, esend, erecv, s1, r1, s2, r2, s3, r3,
):
    r, c = lax.axis_index("rows"), lax.axis_index("cols")
    count, size, _ = wl.shape
    width = ortho.shape[1]
    body = count * size
    piece = got2.shape[1]

    weights = fetch_blocks((lower, diag, upper, inverse), (wl, wd, wu, wi), wsem, c)

    def at(i):
        return pl.ds(pl.multiple_of(i * size, size), size)

    def turn(i, carry):
        oext[at(i), :] = dot(wext[at(i), :], rinv[...]).astype(jnp.bfloat16)
        return carry

    lax.fori_loop(0, count // 2 + 1, turn, 0)

    early = (count // 2) * size

    def columns(start, extent, k):
        return oext.at[pl.ds(size + start, extent), pl.ds(pl.multiple_of(k * width, width), width)]

    def home(start, extent, k):
        return ortho.at[pl.ds(pl.multiple_of(k * body + start, size), extent), :]

    def go_home(start, extent, send, recv):
        there = functools.partial(home, start, extent)
        return exchange(
            "cols", nc, c, functools.partial(columns, start, extent), there, there, send, recv
        )

    finish_early = go_home(0, early, osend, orecv)
    lax.fori_loop(count // 2 + 1, count + 2, turn, 0)
    own = pltpu.make_async_copy(columns(0, body, c), home(0, body, c), lsem)
    own.start()
    total[...] = jnp.zeros_like(total)
    for copy in weights:
        copy.wait()

    def block(i, carry):
        image = apply_block(i, size, oext, wl, wd, wu, wi)
        total[...] += inner(oext[at(i + 1), :], image)
        return carry

    lax.fori_loop(0, count, block, 0)

    def slab(k):
        return pl.ds(pl.multiple_of(k * width, width), width)

    bit, used = 1, 0
    kept = list(range(0, nc))
    while bit < nc:
        peer = flip(c, bit)
        kept = [k for k in kept if k & bit == 0]
        copies = [
            remote(
                total.at[:, slab(flips(peer, k))], got1.at[used + n], s1.at[used + n], r1.at[used + n],
                cols=peer,
            )
            for n, k in enumerate(kept)
        ]
        for copy in copies:
            copy.start()
        if 2 * bit == nc:
            finish_late = go_home(early, body - early, esend, erecv)
        for n, (k, copy) in enumerate(zip(kept, copies)):
            copy.wait()
            where = slab(flips(c, k))
            if 2 * bit == nc:
                part[...] = total[:, where] + got1[used + n]
            else:
                total[:, where] = total[:, where] + got1[used + n]
        used += len(kept)
        bit *= 2

    def tile(ref, k):
        return ref.at[pl.ds(pl.multiple_of(k * piece, 8), piece), :]

    finish = exchange(
        "rows", nr, r, lambda d: tile(part, d), lambda k: got2.at[k], lambda k: got2.at[k], s2, r2
    )
    got2[r] = part[pl.ds(pl.multiple_of(r * piece, 8), piece), :]
    finish()
    projected[pl.ds(pl.multiple_of(r * piece, 8), piece), :] = sum(
        (got2[k] for k in range(1, nr)), got2[0]
    )
    exchange(
        "rows", nr, r, lambda d: tile(projected, r), lambda k: tile(projected, r),
        lambda k: tile(projected, k), s3, r3,
    )()
    own.wait()
    finish_early()
    finish_late()


def shards(nr, nc, basis, lower, diag, upper, inverse):
    blocks, size, _ = diag.shape
    width = basis.shape[1]
    order = width * nc
    count = blocks // nc
    across = order // LANES
    tiles = across * (across + 1) // 2 * LANES // 8
    piece = -(-tiles // (nr * nc)) * 8
    share = piece * nr
    dma = pltpu.SemaphoreType.DMA
    held = [pltpu.VMEM((count, size, size), jnp.bfloat16)] * 4
    extended = ((count + 2) * size, order)
    pair = lambda n: [dma((n,)), dma((n,))]
    kinds = count // CHUNK + 2
    opflops = 8 * count * size * size * order + 2 * count * size * order * order

    wext, gram = pl.pallas_call(
        functools.partial(front_kernel, nr, nc),
        out_shape=(
            jax.ShapeDtypeStruct(extended, jnp.bfloat16),
            jax.ShapeDtypeStruct((nc * share, LANES), jnp.float32),
        ),
        in_specs=[ANY] * 5,
        out_specs=(VMEM, VMEM),
        scratch_shapes=[pltpu.VMEM(extended, jnp.bfloat16)] + held + [
            pltpu.VMEM((order, order), jnp.float32),
            pltpu.VMEM((nc * share, LANES), jnp.float32),
            pltpu.VMEM((nc, share, LANES), jnp.float32),
            pltpu.VMEM((share, LANES), jnp.float32),
            pltpu.VMEM((nr, piece, LANES), jnp.float32),
            dma((4,)), dma((kinds,)), dma((kinds, nc)), dma((kinds, nc)), dma((2,)), dma((2,)),
        ] + pair(nc) + pair(nr) + pair(nr) + pair(nc),
        compiler_params=pltpu.CompilerParams(has_side_effects=True),
        cost_estimate=pl.CostEstimate(flops=opflops, bytes_accessed=1 << 23, transcendentals=0),
        name="front",
    )(basis, lower, diag, upper, inverse)

    rinv = inverse_upper(gram, order)

    lines = order // nr
    return pl.pallas_call(
        functools.partial(back_kernel, nr, nc),
        out_shape=(
            jax.ShapeDtypeStruct(basis.shape, jnp.bfloat16),
            jax.ShapeDtypeStruct((order, width), jnp.float32),
        ),
        in_specs=[VMEM, VMEM] + [ANY] * 4,
        out_specs=(ANY, VMEM),
        scratch_shapes=[pltpu.VMEM(extended, jnp.bfloat16)] + held + [
            pltpu.VMEM((order, order), jnp.float32),
            pltpu.VMEM((nc, order, width), jnp.float32),
            pltpu.VMEM((order, width), jnp.float32),
            pltpu.VMEM((nr, lines, width), jnp.float32),
            dma((4,)), dma,
        ] + pair(nc) + pair(nc) + pair(nc) + pair(nr) + pair(nr),
        compiler_params=pltpu.CompilerParams(has_side_effects=True),
        cost_estimate=pl.CostEstimate(flops=opflops, bytes_accessed=1 << 23, transcendentals=0),
        name="back",
    )(wext, rinv, lower, diag, upper, inverse)


def solution(mesh):
    in_specs = (
        P("rows", "cols"),
        P("rows", None, None),
        P("rows", None, None),
        P("rows", None, None),
        P("rows", None, None),
    )
    out_specs = (P("rows", "cols"), P(None, "cols"))
    body = functools.partial(shards, mesh.shape["rows"], mesh.shape["cols"])
    return jax.shard_map(body, mesh=mesh, in_specs=in_specs, out_specs=out_specs, check_vma=False)
```
